128 devices in a mesh: cx: 8 (over y, core), cy: 16 (over z, x).
Axes of the slice: x: 4, y: 4, z: 4, core: 2. Of those that a mesh axis runs over, the one named last changes fastest.
Arguments:
- queries: bfloat16 [24576, 4096], P(('cx', 'cy')), may hold values from -300 to 300
- keys: bfloat16 [131072, 512], P(('cx', 'cy')), may hold values from -6 to 6
- values: bfloat16 [131072, 512], P(('cx', 'cy')), may hold values from -6 to 6
- d_out: bfloat16 [24576, 4096], P(('cx', 'cy')), may hold values from -6 to 6
- selection: int32 [384, 4, 16], replicated, may hold values from 0 to 1663, as said below
Outputs:
- d_queries: float32 [24576, 4096], P(('cx', 'cy'))
- d_keys: float32 [131072, 512], P(('cx', 'cy'))
- d_values: float32 [131072, 512], P(('cx', 'cy'))
The draws below stay inside these ranges and needn't reach their ends.
Inputs may be any that keep to these rules, and one draw needn't show every extreme that they name: `selection`: every entry is a block below 1664. Over the 3 consecutive query blocks of one device (rows d * 3 to d * 3 + 2) all 192 entries differ, and at most 2 of them lie in the blocks k * 16 to k * 16 + 15 of any one k; that most is reached on every device.
All inputs are finite; a program needn't handle non-finite values.
Results may differ from the reference program's by a relative error of at most 0.0042.
Values may be sent and summed in bfloat16 or wider, within the bound.
A program may use at most 192 MiB of HBM per device.

```python
import jax
import jax.numpy as jnp
from jax import lax

H = 32
KVH = 4
HD = 128
BLK = 64
TOPK = 16
KB_DEV = 16
GROUP = 8
NB = 2048
NQB = 384
SEQ = 131072
NQ = 24576
PICKS = 192
VALID = 104
CAP = 2
DEVICES = 128


def selection_table(key):
    base = jax.random.fold_in(key, 11)
    first_key, second_key, third_key = jax.random.split(base, 3)
    candidates = VALID * CAP
    owner_of = jnp.arange(candidates, dtype=jnp.int32) // CAP
    raw = jax.random.randint(first_key, (DEVICES, candidates), 0, 2 ** 20)
    bucket = 1 + owner_of // max(1, VALID // 8)
    score = raw // bucket * candidates + jnp.arange(candidates, dtype=jnp.int32)
    unused, chosen = lax.top_k(score, PICKS)
    order_score = jax.random.randint(second_key, (DEVICES, PICKS), 0, 2 ** 20) * PICKS + jnp.arange(PICKS, dtype=jnp.int32)
    order = jnp.argsort(order_score, axis=1)
    chosen = jnp.take_along_axis(chosen, order, axis=1)
    owner = chosen // CAP
    copy_index = chosen % CAP
    offset = copy_index + CAP * jax.random.randint(third_key, (DEVICES, PICKS), 0, KB_DEV // CAP)
    return (owner * KB_DEV + offset).reshape(NQB, KVH, TOPK).astype(jnp.int32)


def key_table(key):
    return jnp.clip(jax.random.normal(jax.random.fold_in(key, 21), (SEQ, KVH * HD), jnp.float32), -6.0, 6.0)


def draw_selection(key, part):
    return selection_table(key)


def draw_keys(key, part):
    return key_table(key).astype(jnp.bfloat16)


def draw_queries(key, part):
    result = jax.random.normal(jax.random.fold_in(key, 31), (NQ, H * HD), jnp.float32)
    return jnp.clip(result, -300.0, 300.0).astype(jnp.bfloat16)


def block_scale(stream_key, shape, cuts, smallest, high):
    loudness = 1.0
    for dim, parts in cuts:
        steps = jax.random.uniform(jax.random.fold_in(jax.random.fold_in(stream_key, 6), dim), (parts,), jnp.float32, smallest / len(cuts), high / len(cuts))
        loudness = loudness * jnp.repeat(jnp.exp(steps), shape[dim] // parts).reshape((-1,) + (1,) * (len(shape) - 1 - dim))
    return loudness


def bell_draw(own_key, dims, deviation, bound, shards=(), held_as=jnp.bfloat16):
    entries = jax.random.normal(own_key, dims, jnp.float32) * deviation
    if len(shards) > 0:
        entries = block_scale(own_key, dims, shards, -0.22, 0.18) * entries
    return jnp.clip(entries, min=-bound, max=bound).astype(held_as)


def setup_inputs(seed: int = 0) -> dict:
    key_list = jax.random.split(jax.random.key(seed), 6)
    return {
        "queries": draw_queries(jax.random.fold_in(key_list[5], 71), 0),
        "keys": draw_keys(jax.random.fold_in(key_list[5], 71), 0),
        "values": bell_draw(key_list[2], (SEQ, KVH * HD), 1.0, 6.0, ((0, 128),)),
        "d_out": bell_draw(key_list[3], (NQ, H * HD), 1.0, 6.0, ((0, 128),)),
        "selection": draw_selection(jax.random.fold_in(key_list[5], 71), 0),
    }


def rounded(value):
    return lax.optimization_barrier(value.astype(jnp.bfloat16)).astype(jnp.float32)


def block_grads(q_rows, o_rows, key_rows, value_rows):
    scale = HD ** -0.5
    highest = lax.Precision.HIGHEST
    scores = jnp.einsum("agzd,gkd->gzak", q_rows, key_rows, precision=highest) * scale
    probs = jax.nn.softmax(scores, axis=-1)
    probs_half = rounded(probs)
    d_probs = jnp.einsum("agzd,gkd->gzak", o_rows, value_rows, precision=highest)
    delta = jnp.sum(probs * d_probs, axis=-1, keepdims=True)
    d_scores = rounded(probs * (d_probs - delta))
    d_query = jnp.einsum("gzak,gkd->agzd", d_scores, key_rows, precision=highest) * scale
    d_key = jnp.einsum("gzak,agzd->gkd", d_scores, q_rows, precision=highest) * scale
    d_value = jnp.einsum("gzak,agzd->gkd", probs_half, o_rows, precision=highest)
    return d_query, d_key, d_value


def reference(queries, keys, values, d_out, selection):
    keys4 = keys.astype(jnp.float32).reshape(NB, BLK, KVH, HD)
    values4 = values.astype(jnp.float32).reshape(NB, BLK, KVH, HD)
    q_blocks = queries.reshape(NQB, BLK, KVH, GROUP, HD)
    o_blocks = d_out.reshape(NQB, BLK, KVH, GROUP, HD)
    head_index = jnp.arange(KVH, dtype=jnp.int32)[:, None]

    def step(carry, inputs):
        d_keys_all, d_values_all = carry
        q_rows, o_rows, chosen = inputs
        key_rows = keys4[chosen, :, head_index, :].reshape(KVH, TOPK * BLK, HD)
        value_rows = values4[chosen, :, head_index, :].reshape(KVH, TOPK * BLK, HD)
        d_query, d_key, d_value = block_grads(q_rows.astype(jnp.float32), o_rows.astype(jnp.float32), key_rows, value_rows)
        d_keys_all = d_keys_all.at[chosen, :, head_index, :].add(d_key.reshape(KVH, TOPK, BLK, HD))
        d_values_all = d_values_all.at[chosen, :, head_index, :].add(d_value.reshape(KVH, TOPK, BLK, HD))
        return (d_keys_all, d_values_all), d_query

    start = (jnp.zeros((NB, BLK, KVH, HD), jnp.float32), jnp.zeros((NB, BLK, KVH, HD), jnp.float32))
    (d_keys_all, d_values_all), d_queries = lax.scan(step, start, (q_blocks, o_blocks, selection))
    return (d_queries.reshape(NQ, H * HD), d_keys_all.reshape(SEQ, KVH * HD), d_values_all.reshape(SEQ, KVH * HD))
```

```python
import jax
import jax.numpy as jnp
from jax import lax
from jax.experimental import pallas as pl
from jax.experimental.pallas import tpu as pltpu
from jax.sharding import PartitionSpec as P

H = 32
KVH = 4
HD = 128
BLK = 64
TOPK = 16
QB_DEV = 3
KB_DEV = 16
GROUP = 8
PICKS = 192
CAP = 2
DEVICES = 128
VALID = DEVICES * (KB_DEV - QB_DEV) // KB_DEV
SLOTS = VALID * CAP
TILES = KB_DEV * KVH
SETS = QB_DEV * KVH
KEYS = TOPK * BLK
ROWS = GROUP * BLK
CHUNK = 256
CHUNKS = KEYS // CHUNK
UNROLL = True
SCALE = HD**-0.5
EXP2_SCALE = SCALE * 1.4426950408889634
MESH = pl.DeviceIdType.MESH
MIB = 1024 * 1024


def fill_tables(me, picks, tile_of, pick_of, chosen):
    rows = lax.broadcasted_iota(jnp.int32, (DEVICES, PICKS), 0)
    chosen[...] = jnp.sum(jnp.where(rows == me, picks, 0), axis=0, keepdims=True)
    shape = (PICKS, DEVICES)
    position = lax.broadcasted_iota(jnp.int32, shape, 0)
    device = lax.broadcasted_iota(jnp.int32, shape, 1)
    block = picks.T
    mine = block // KB_DEV == me
    code = position * TILES + block % KB_DEV * KVH + position // TOPK % KVH
    big = PICKS * TILES
    first = jnp.min(jnp.where(mine, code, big), axis=0, keepdims=True)
    last = jnp.max(jnp.where(mine, code, -1), axis=0, keepdims=True)
    tile_of[0:1, :] = jnp.where(first < big, first % TILES, TILES)
    tile_of[1:2, :] = jnp.where(last > first, last % TILES, TILES)
    own = jnp.sum(jnp.where(device == me, block, 0), axis=1, keepdims=True)
    held = own // KB_DEV == device
    pick_of[0:1, :] = jnp.min(jnp.where(held, position, PICKS - 1), axis=0, keepdims=True)
    pick_of[1:2, :] = jnp.max(jnp.where(held, position, 0), axis=0, keepdims=True)


STRIDES = [(a, b) for b in range(4) for a in range(4)]
ROUNDS = DEVICES // len(STRIDES)


def exchange_kernel(
    picks_hbm, q_hbm, k_hbm, v_hbm, o_hbm,
    dq_hbm, gk_hbm, gv_hbm, tile_hbm,
    picks, tile_v, pick_v, chosen_v, tile_of, pick_of, chosen,
    kl, vl, sendk, sendv, rk, rv, q_s, o_s, e_s, inv_s, dp_s, kg, vg, qg, og,
    terms, dq_acc, dq_s,
    load_sem, send_sem, recv_sem, own_sem,
):
    cx, cy = lax.axis_index("cx"), lax.axis_index("cy")
    me = cx * 16 + cy
    at_x = [(cy + a) % 4 for a in range(4)]
    at_z = [(cy // 4 + b) % 4 * 4 for b in range(4)]

    def peers(turn):
        core = (cx + turn // 4) % 2
        y = [(cx // 2 + turn % 4 + e) % 4 * 2 + core for e in range(4)]
        return [(y[(a + b) % 4], at_z[(a + b) % 4] + at_x[a]) for a, b in STRIDES]

    def load_tiles(src, dst, sem):
        def body(t, carry):
            rows = pl.ds(pl.multiple_of(t // KVH * BLK, BLK), BLK)
            lanes = pl.ds(pl.multiple_of(t % KVH * HD, HD), HD)
            pltpu.make_async_copy(src.at[rows, lanes], dst.at[t], sem).start()
            return carry

        lax.fori_loop(0, TILES, body, 0)

    def wait_bytes(ref, sem):
        pltpu.make_async_copy(ref, ref, sem).wait()

    def greet(turn, carry):
        for n, device in enumerate(peers(turn)):

            @pl.when((turn > 0) | (n > 0))
            def _():
                pl.semaphore_signal(barrier, inc=1, device_id=device, device_id_type=MESH)

        return carry

    barrier = pltpu.get_barrier_semaphore()
    load_picks = pltpu.make_async_copy(picks_hbm, picks, load_sem.at[4])
    load_picks.start()
    lax.fori_loop(0, ROUNDS, greet, 0)
    load_tiles(k_hbm, kl, load_sem.at[0])
    load_tiles(v_hbm, vl, load_sem.at[1])
    load_q = pltpu.make_async_copy(q_hbm, q_s, load_sem.at[2])
    load_o = pltpu.make_async_copy(o_hbm, o_s, load_sem.at[3])
    load_q.start()
    load_o.start()
    load_picks.wait()
    fill_tables(me, picks[...], tile_v, pick_v, chosen_v)
    moves = [
        pltpu.make_async_copy(tile_v, tile_of, load_sem.at[4]),
        pltpu.make_async_copy(pick_v, pick_of, load_sem.at[5]),
        pltpu.make_async_copy(chosen_v, chosen, load_sem.at[6]),
        pltpu.make_async_copy(tile_v, tile_hbm, load_sem.at[7]),
    ]
    for move in moves:
        move.start()

    def forward_copy(send, got, index, device):
        return pltpu.make_async_remote_copy(
            src_ref=send.at[pl.ds(CAP * (device[0] * 16 + device[1]), CAP)],
            dst_ref=got.at[pl.ds(CAP * me, CAP)],
            send_sem=send_sem.at[index],
            recv_sem=recv_sem.at[index],
            device_id=device,
            device_id_type=MESH,
        )

    def forward(local, send, got, index):
        @pl.when(me < VALID)
        def _():
            for c in range(CAP):
                tile = jnp.minimum(tile_of[c, me], TILES - 1)
                got[me * CAP + c] = local[tile]

            def body(turn, carry):
                devices = peers(turn)
                for a, b in devices:
                    for c in range(CAP):
                        tile = jnp.minimum(tile_of[c, a * 16 + b], TILES - 1)
                        send[(a * 16 + b) * CAP + c] = local[tile]
                for n, device in enumerate(devices):

                    @pl.when((turn > 0) | (n > 0))
                    def _():
                        forward_copy(send, got, index, device).start()

                return carry

            lax.fori_loop(0, ROUNDS, body, 0)

    def wait_forward(got, index):
        @pl.when(me < VALID)
        def _():
            wait_bytes(got.at[pl.ds(0, SLOTS - CAP)], recv_sem.at[index])

        @pl.when(me >= VALID)
        def _():
            wait_bytes(got, recv_sem.at[index])

    def gather(got, dst, group):
        def body(j, carry):
            rows = pl.ds(pl.multiple_of(j * BLK, BLK), BLK)
            owner = chosen[0, group * TOPK + j] // KB_DEV
            later = (pick_of[0, owner] != group * TOPK + j).astype(jnp.int32)
            dst[rows, :] = got[owner * CAP + later]
            return carry

        lax.fori_loop(0, TOPK, body, 0)

    def rows_of(src, dst, group):
        b, g = group // KVH, group % KVH
        rows = pl.ds(pl.multiple_of(b * BLK, BLK), BLK)
        for h in range(GROUP):
            lanes = pl.ds(pl.multiple_of((g * GROUP + h) * HD, HD), HD)
            dst[h * BLK : (h + 1) * BLK, :] = src[rows, lanes]

    def chunk(c):
        return pl.ds(pl.multiple_of(c * CHUNK, CHUNK), CHUNK)

    def first_phase(group, carry):
        rows_of(q_s, qg, group)
        rows_of(o_s, og, group)
        gather(rk, kg, group)

        def score(c, top):
            s = lax.dot_general(
                kg[chunk(c), :], qg[...], (((1,), (1,)), ((), ())),
                preferred_element_type=jnp.float32,
            )
            e_s[group, chunk(c), :] = s
            return jnp.maximum(top, jnp.max(s, axis=0, keepdims=True))

        top = lax.fori_loop(
            0, CHUNKS, score, jnp.full((1, ROWS), -jnp.inf, jnp.float32), unroll=UNROLL
        )

        def exponent(c, total):
            e = jnp.exp2((e_s[group, chunk(c), :] - top) * EXP2_SCALE)
            e_s[group, chunk(c), :] = e
            return total + jnp.sum(e, axis=0, keepdims=True)

        total = lax.fori_loop(
            0, CHUNKS, exponent, jnp.zeros((1, ROWS), jnp.float32), unroll=UNROLL
        )
        inverse = 1.0 / total
        inv_s[group] = inverse

        def value_terms(c, carry):
            p = (e_s[group, chunk(c), :] * inverse).astype(jnp.bfloat16)
            dv = jnp.dot(p, og[...], preferred_element_type=jnp.float32)
            n = CHUNK // BLK
            terms[pl.ds(group * TOPK + c * n, n)] = dv.astype(jnp.bfloat16).reshape(n, BLK, HD)
            return carry

        return lax.fori_loop(0, CHUNKS, value_terms, carry, unroll=UNROLL)

    def second_phase(group, carry):
        rows_of(q_s, qg, group)
        rows_of(o_s, og, group)
        gather(rk, kg, group)
        gather(rv, vg, group)

        def d_prob(c, delta):
            dp = lax.dot_general(
                vg[chunk(c), :], og[...], (((1,), (1,)), ((), ())),
                preferred_element_type=jnp.float32,
            )
            dp_s[chunk(c), :] = dp
            return delta + jnp.sum(e_s[group, chunk(c), :] * dp, axis=0, keepdims=True)

        delta = lax.fori_loop(
            0, CHUNKS, d_prob, jnp.zeros((1, ROWS), jnp.float32), unroll=UNROLL
        )
        inverse = inv_s[group]
        delta = delta * inverse
        dq_acc[...] = jnp.zeros_like(dq_acc)

        def key_terms(c, carry):
            p = e_s[group, chunk(c), :] * inverse
            ds = (p * (dp_s[chunk(c), :] - delta)).astype(jnp.bfloat16)
            dk = jnp.dot(ds, qg[...], preferred_element_type=jnp.float32) * SCALE
            n = CHUNK // BLK
            terms[pl.ds(group * TOPK + c * n, n)] = dk.astype(jnp.bfloat16).reshape(n, BLK, HD)
            dq_acc[...] += lax.dot_general(
                ds, kg[chunk(c), :], (((0,), (0,)), ((), ())),
                preferred_element_type=jnp.float32,
            )
            return carry

        lax.fori_loop(0, CHUNKS, key_terms, 0, unroll=UNROLL)
        b, g = group // KVH, group % KVH
        rows = pl.ds(pl.multiple_of(b * BLK, BLK), BLK)
        for h in range(GROUP):
            lanes = pl.ds(pl.multiple_of((g * GROUP + h) * HD, HD), HD)
            dq_s[rows, lanes] = dq_acc[h * BLK : (h + 1) * BLK, :] * SCALE
        return carry

    def back_copy(send, got, index, device):
        return pltpu.make_async_remote_copy(
            src_ref=send.at[pl.ds(CAP * (device[0] * 16 + device[1]), CAP)],
            dst_ref=got.at[pl.ds(CAP * me, CAP)],
            send_sem=send_sem.at[index],
            recv_sem=recv_sem.at[index],
            device_id=device,
            device_id_type=MESH,
        )

    def backward(send, got, index):
        def body(turn, carry):
            devices = peers(turn)
            for a, b in devices:
                for c in range(CAP):
                    send[(a * 16 + b) * CAP + c] = terms[pick_of[c, a * 16 + b]]
            for n, device in enumerate(devices):

                @pl.when(((turn > 0) | (n > 0)) & (device[0] * 16 + device[1] < VALID))
                def _():
                    back_copy(send, got, index, device).start()

            return carry

        lax.fori_loop(0, ROUNDS, body, 0)

        @pl.when(me < VALID)
        def _():
            own = pl.ds(CAP * me, CAP)
            pltpu.make_async_copy(send.at[own], got.at[own], own_sem.at[index - 2]).start()

    def wait_backward(send, got, index):
        @pl.when(me < VALID)
        def _():
            own = pl.ds(CAP * me, CAP)
            pltpu.make_async_copy(send.at[own], got.at[own], own_sem.at[index - 2]).wait()
            wait_bytes(got.at[pl.ds(0, (DEVICES - 1) * CAP)], recv_sem.at[index])
            wait_bytes(send.at[pl.ds(0, SLOTS - CAP)], send_sem.at[index])

        @pl.when(me >= VALID)
        def _():
            wait_bytes(send.at[pl.ds(0, SLOTS)], send_sem.at[index])

    def wait_sent(send, index):
        @pl.when(me < VALID)
        def _():
            wait_bytes(send.at[pl.ds(0, (DEVICES - 1) * CAP)], send_sem.at[index])

    for move in moves:
        move.wait()
    wait_bytes(kl, load_sem.at[0])
    pl.semaphore_wait(barrier, DEVICES - 1)
    forward(kl, sendk, rk, 0)
    wait_bytes(vl, load_sem.at[1])
    forward(vl, sendv, rv, 1)
    load_q.wait()
    load_o.wait()
    wait_forward(rk, 0)
    lax.fori_loop(0, SETS, first_phase, 0)
    wait_sent(sendk, 0)
    backward(sendk, gv_hbm, 2)
    wait_forward(rv, 1)
    lax.fori_loop(0, SETS, second_phase, 0)
    wait_sent(sendv, 1)
    backward(sendv, gk_hbm, 3)
    store_dq = pltpu.make_async_copy(dq_s, dq_hbm, load_sem.at[2])
    store_dq.start()
    wait_backward(sendk, gv_hbm, 2)
    wait_backward(sendv, gk_hbm, 3)
    store_dq.wait()


def exchange(picks, queries, keys, values, d_out):
    anywhere = pl.BlockSpec(memory_space=pl.ANY)
    half, full = jnp.bfloat16, jnp.float32
    table = jax.ShapeDtypeStruct((CAP, DEVICES), jnp.int32)
    back = jax.ShapeDtypeStruct((DEVICES * CAP, BLK, HD), half)
    return pl.pallas_call(
        exchange_kernel,
        out_shape=(jax.ShapeDtypeStruct((QB_DEV * BLK, H * HD), full), back, back, table),
        in_specs=[anywhere] * 5,
        out_specs=[anywhere] * 4,
        scratch_shapes=[
            pltpu.VMEM((DEVICES, PICKS), jnp.int32),
            pltpu.VMEM((CAP, DEVICES), jnp.int32),
            pltpu.VMEM((CAP, DEVICES), jnp.int32),
            pltpu.VMEM((1, PICKS), jnp.int32),
            pltpu.SMEM((CAP, DEVICES), jnp.int32),
            pltpu.SMEM((CAP, DEVICES), jnp.int32),
            pltpu.SMEM((1, PICKS), jnp.int32),
            pltpu.VMEM((TILES, BLK, HD), half),
            pltpu.VMEM((TILES, BLK, HD), half),
            pltpu.VMEM((DEVICES * CAP, BLK, HD), half),
            pltpu.VMEM((DEVICES * CAP, BLK, HD), half),
            pltpu.VMEM((SLOTS, BLK, HD), half),
            pltpu.VMEM((SLOTS, BLK, HD), half),
            pltpu.VMEM((QB_DEV * BLK, H * HD), half),
            pltpu.VMEM((QB_DEV * BLK, H * HD), half),
            pltpu.VMEM((SETS, KEYS, ROWS), full),
            pltpu.VMEM((SETS, 1, ROWS), full),
            pltpu.VMEM((KEYS, ROWS), full),
            pltpu.VMEM((KEYS, HD), half),
            pltpu.VMEM((KEYS, HD), half),
            pltpu.VMEM((ROWS, HD), half),
            pltpu.VMEM((ROWS, HD), half),
            pltpu.VMEM((PICKS, BLK, HD), half),
            pltpu.VMEM((ROWS, HD), full),
            pltpu.VMEM((QB_DEV * BLK, H * HD), full),
            pltpu.SemaphoreType.DMA((8,)),
            pltpu.SemaphoreType.DMA((4,)),
            pltpu.SemaphoreType.DMA((4,)),
            pltpu.SemaphoreType.DMA((2,)),
        ],
        compiler_params=pltpu.CompilerParams(
            collective_id=0, has_side_effects=True, vmem_limit_bytes=62 * MIB
        ),
    )(picks, queries, keys, values, d_out)


FOLD = 32
STEPS = DEVICES * CAP // FOLD


def collect_kernel(
    tile_of, gk, gv, dq_hbm, dq_out, dk_out, dv_out, dk, dk2, dv, dv2, dq, sems
):
    step = pl.program_id(0)
    load = pltpu.make_async_copy(dq_hbm, dq, sems.at[2])
    store = pltpu.make_async_copy(dq, dq_out, sems.at[3])

    @pl.when(step == 0)
    def _():
        load.start()
        for total in (dk, dk2, dv, dv2):
            total[...] = jnp.zeros_like(total)

    @pl.when(step == STEPS // 2)
    def _():
        load.wait()
        store.start()

    def add(i, carry):
        device = step * (FOLD // CAP) + i
        tile, tile2 = tile_of[0, device], tile_of[1, device]
        dk[tile] += gk[CAP * i].astype(jnp.float32)
        dk2[tile2] += gk[CAP * i + 1].astype(jnp.float32)
        dv[tile] += gv[CAP * i].astype(jnp.float32)
        dv2[tile2] += gv[CAP * i + 1].astype(jnp.float32)
        return carry

    lax.fori_loop(0, FOLD // CAP, add, 0, unroll=4)

    @pl.when(step == STEPS - 1)
    def _():
        def put(t, carry):
            rows = pl.ds(pl.multiple_of(t // KVH * BLK, BLK), BLK)
            lanes = pl.ds(pl.multiple_of(t % KVH * HD, HD), HD)
            dk[t] += dk2[t]
            dv[t] += dv2[t]
            pltpu.make_async_copy(dk.at[t], dk_out.at[rows, lanes], sems.at[0]).start()
            pltpu.make_async_copy(dv.at[t], dv_out.at[rows, lanes], sems.at[1]).start()
            return carry

        lax.fori_loop(0, TILES, put, 0)
        pltpu.make_async_copy(dk_out, dk_out, sems.at[0]).wait()
        pltpu.make_async_copy(dv_out, dv_out, sems.at[1]).wait()
        store.wait()


def collect(tile_of, gk, gv, d_queries):
    full = jnp.float32
    shape = jax.ShapeDtypeStruct((KB_DEV * BLK, KVH * HD), full)
    part = pl.BlockSpec((FOLD, BLK, HD), lambda i: (i, 0, 0))
    anywhere = pl.BlockSpec(memory_space=pl.ANY)
    return pl.pallas_call(
        collect_kernel,
        grid=(STEPS,),
        out_shape=(jax.ShapeDtypeStruct(d_queries.shape, full), shape, shape),
        in_specs=[pl.BlockSpec(memory_space=pltpu.SMEM), part, part, anywhere],
        out_specs=[anywhere] * 3,
        scratch_shapes=[pltpu.VMEM((TILES + 1, BLK, HD), full)] * 4
        + [pltpu.VMEM(d_queries.shape, full), pltpu.SemaphoreType.DMA((4,))],
        compiler_params=pltpu.CompilerParams(vmem_limit_bytes=62 * MIB),
    )(tile_of, gk, gv, d_queries)


def body(queries, keys, values, d_out, selection):
    picks = selection.reshape(DEVICES, PICKS)
    d_queries, gk, gv, tile_of = exchange(picks, queries, keys, values, d_out)
    return collect(tile_of, gk, gv, d_queries)


def solution(mesh):
    rows = P(("cx", "cy"), None)
    return jax.shard_map(
        body,
        mesh=mesh,
        in_specs=(rows, rows, rows, rows, P()),
        out_specs=(rows, rows, rows),
        check_vma=False,
    )
```

```python
import jax
import jax.numpy as jnp
from jax import lax
from jax.experimental import pallas as pl
from jax.experimental.pallas import tpu as pltpu
from jax.sharding import PartitionSpec as P

H = 32
KVH = 4
HD = 128
BLK = 64
TOPK = 16
QB_DEV = 3
KB_DEV = 16
GROUP = 8
PICKS = 192
CAP = 2
DEVICES = 128
VALID = DEVICES * (KB_DEV - QB_DEV) // KB_DEV
SLOTS = VALID * CAP
TILES = KB_DEV * KVH
SETS = QB_DEV * KVH
KEYS = TOPK * BLK
ROWS = GROUP * BLK
CHUNK = 256
CHUNKS = KEYS // CHUNK
UNROLL = True
SCALE = HD**-0.5
EXP2_SCALE = SCALE * 1.4426950408889634
MESH = pl.DeviceIdType.MESH
MIB = 1024 * 1024


def fill_tables(me, picks, tile_of, pick_of, chosen):
    rows = lax.broadcasted_iota(jnp.int32, (DEVICES, PICKS), 0)
    chosen[...] = jnp.sum(jnp.where(rows == me, picks, 0), axis=0, keepdims=True)
    shape = (PICKS, DEVICES)
    position = lax.broadcasted_iota(jnp.int32, shape, 0)
    device = lax.broadcasted_iota(jnp.int32, shape, 1)
    block = picks.T
    mine = block // KB_DEV == me
    code = position * TILES + block % KB_DEV * KVH + position // TOPK % KVH
    big = PICKS * TILES
    first = jnp.min(jnp.where(mine, code, big), axis=0, keepdims=True)
    last = jnp.max(jnp.where(mine, code, -1), axis=0, keepdims=True)
    tile_of[0:1, :] = jnp.where(first < big, first % TILES, TILES)
    tile_of[1:2, :] = jnp.where(last > first, last % TILES, TILES)
    own = jnp.sum(jnp.where(device == me, block, 0), axis=1, keepdims=True)
    held = own // KB_DEV == device
    pick_of[0:1, :] = jnp.min(jnp.where(held, position, PICKS - 1), axis=0, keepdims=True)
    pick_of[1:2, :] = jnp.max(jnp.where(held, position, 0), axis=0, keepdims=True)


STRIDES = [(a, b) for b in range(4) for a in range(4)]
ROUNDS = DEVICES // len(STRIDES)


def exchange_kernel(
    picks_hbm, q_hbm, k_hbm, v_hbm, o_hbm,
    dq_hbm, gk_hbm, gv_hbm, tile_hbm,
    picks, tile_v, pick_v, chosen_v, tile_of, pick_of, chosen,
    kl, vl, sendk, sendv, rk, rv, q_s, o_s, e_s, inv_s, dp_s, kg, vg, qg, og,
    terms, dq_acc, dq_s,
    load_sem, send_sem, recv_sem, own_sem,
):
    cx, cy = lax.axis_index("cx"), lax.axis_index("cy")
    me = cx * 16 + cy
    sign = 1 + 2 * (cx % 2)
    at_x = [(cy + a * sign) % 4 for a in range(4)]
    at_z = [(cy // 4 + b * sign) % 4 * 4 for b in range(4)]

    def peers(turn):
        core = (cx + turn // 4) % 2
        y = [(cx // 2 + (turn % 4 + e) * sign) % 4 * 2 + core for e in range(4)]
        return [(y[(a + b) % 4], at_z[(a + b) % 4] + at_x[a]) for a, b in STRIDES]

    def load_tiles(src, dst, sem):
        def body(t, carry):
            rows = pl.ds(pl.multiple_of(t // KVH * BLK, BLK), BLK)
            lanes = pl.ds(pl.multiple_of(t % KVH * HD, HD), HD)
            pltpu.make_async_copy(src.at[rows, lanes], dst.at[t], sem).start()
            return carry

        lax.fori_loop(0, TILES, body, 0)

    def wait_bytes(ref, sem):
        pltpu.make_async_copy(ref, ref, sem).wait()

    def greet(turn, carry):
        for n, device in enumerate(peers(turn)):

            @pl.when((turn > 0) | (n > 0))
            def _():
                pl.semaphore_signal(barrier, inc=1, device_id=device, device_id_type=MESH)

        return carry

    barrier = pltpu.get_barrier_semaphore()
    load_picks = pltpu.make_async_copy(picks_hbm, picks, load_sem.at[4])
    load_picks.start()
    lax.fori_loop(0, ROUNDS, greet, 0)
    load_tiles(k_hbm, kl, load_sem.at[0])
    load_tiles(v_hbm, vl, load_sem.at[1])
    load_q = pltpu.make_async_copy(q_hbm, q_s, load_sem.at[2])
    load_o = pltpu.make_async_copy(o_hbm, o_s, load_sem.at[3])
    load_q.start()
    load_o.start()
    load_picks.wait()
    fill_tables(me, picks[...], tile_v, pick_v, chosen_v)
    moves = [
        pltpu.make_async_copy(tile_v, tile_of, load_sem.at[4]),
        pltpu.make_async_copy(pick_v, pick_of, load_sem.at[5]),
        pltpu.make_async_copy(chosen_v, chosen, load_sem.at[6]),
        pltpu.make_async_copy(tile_v, tile_hbm, load_sem.at[7]),
    ]
    for move in moves:
        move.start()

    def forward_copy(send, got, index, device):
        return pltpu.make_async_remote_copy(
            src_ref=send.at[pl.ds(CAP * (device[0] * 16 + device[1]), CAP)],
            dst_ref=got.at[pl.ds(CAP * me, CAP)],
            send_sem=send_sem.at[index],
            recv_sem=recv_sem.at[index],
            device_id=device,
            device_id_type=MESH,
        )

    def forward(local, send, got, index):
        @pl.when(me < VALID)
        def _():
            for c in range(CAP):
                tile = jnp.minimum(tile_of[c, me], TILES - 1)
                got[me * CAP + c] = local[tile]

            def body(turn, carry):
                devices = peers(turn)
                for a, b in devices:
                    for c in range(CAP):
                        tile = jnp.minimum(tile_of[c, a * 16 + b], TILES - 1)
                        send[(a * 16 + b) * CAP + c] = local[tile]
                for n, device in enumerate(devices):

                    @pl.when((turn > 0) | (n > 0))
                    def _():
                        forward_copy(send, got, index, device).start()

                return carry

            lax.fori_loop(0, ROUNDS, body, 0)

    def wait_forward(got, index):
        @pl.when(me < VALID)
        def _():
            wait_bytes(got.at[pl.ds(0, SLOTS - CAP)], recv_sem.at[index])

        @pl.when(me >= VALID)
        def _():
            wait_bytes(got, recv_sem.at[index])

    def gather(got, dst, group):
        def body(j, carry):
            rows = pl.ds(pl.multiple_of(j * BLK, BLK), BLK)
            owner = chosen[0, group * TOPK + j] // KB_DEV
            later = (pick_of[0, owner] != group * TOPK + j).astype(jnp.int32)
            dst[rows, :] = got[owner * CAP + later]
            return carry

        lax.fori_loop(0, TOPK, body, 0)

    def rows_of(src, dst, group):
        b, g = group // KVH, group % KVH
        rows = pl.ds(pl.multiple_of(b * BLK, BLK), BLK)
        for h in range(GROUP):
            lanes = pl.ds(pl.multiple_of((g * GROUP + h) * HD, HD), HD)
            dst[h * BLK : (h + 1) * BLK, :] = src[rows, lanes]

    def chunk(c):
        return pl.ds(pl.multiple_of(c * CHUNK, CHUNK), CHUNK)

    def first_phase(group, carry):
        rows_of(q_s, qg, group)
        rows_of(o_s, og, group)
        gather(rk, kg, group)

        def score(c, top):
            s = lax.dot_general(
                kg[chunk(c), :], qg[...], (((1,), (1,)), ((), ())),
                preferred_element_type=jnp.float32,
            )
            e_s[group, chunk(c), :] = s
            return jnp.maximum(top, jnp.max(s, axis=0, keepdims=True))

        top = lax.fori_loop(
            0, CHUNKS, score, jnp.full((1, ROWS), -jnp.inf, jnp.float32), unroll=UNROLL
        )

        def exponent(c, total):
            e = jnp.exp2((e_s[group, chunk(c), :] - top) * EXP2_SCALE)
            e_s[group, chunk(c), :] = e
            return total + jnp.sum(e, axis=0, keepdims=True)

        total = lax.fori_loop(
            0, CHUNKS, exponent, jnp.zeros((1, ROWS), jnp.float32), unroll=UNROLL
        )
        inverse = 1.0 / total
        inv_s[group] = inverse

        def value_terms(c, carry):
            p = (e_s[group, chunk(c), :] * inverse).astype(jnp.bfloat16)
            dv = jnp.dot(p, og[...], preferred_element_type=jnp.float32)
            n = CHUNK // BLK
            terms[pl.ds(group * TOPK + c * n, n)] = dv.astype(jnp.bfloat16).reshape(n, BLK, HD)
            return carry

        return lax.fori_loop(0, CHUNKS, value_terms, carry, unroll=UNROLL)

    def second_phase(group, carry):
        rows_of(q_s, qg, group)
        rows_of(o_s, og, group)
        gather(rk, kg, group)
        gather(rv, vg, group)

        def d_prob(c, delta):
            dp = lax.dot_general(
                vg[chunk(c), :], og[...], (((1,), (1,)), ((), ())),
                preferred_element_type=jnp.float32,
            )
            dp_s[chunk(c), :] = dp
            return delta + jnp.sum(e_s[group, chunk(c), :] * dp, axis=0, keepdims=True)

        delta = lax.fori_loop(
            0, CHUNKS, d_prob, jnp.zeros((1, ROWS), jnp.float32), unroll=UNROLL
        )
        inverse = inv_s[group]
        delta = delta * inverse
        dq_acc[...] = jnp.zeros_like(dq_acc)

        def key_terms(c, carry):
            p = e_s[group, chunk(c), :] * inverse
            ds = (p * (dp_s[chunk(c), :] - delta)).astype(jnp.bfloat16)
            dk = jnp.dot(ds, qg[...], preferred_element_type=jnp.float32) * SCALE
            n = CHUNK // BLK
            terms[pl.ds(group * TOPK + c * n, n)] = dk.astype(jnp.bfloat16).reshape(n, BLK, HD)
            dq_acc[...] += lax.dot_general(
                ds, kg[chunk(c), :], (((0,), (0,)), ((), ())),
                preferred_element_type=jnp.float32,
            )
            return carry

        lax.fori_loop(0, CHUNKS, key_terms, 0, unroll=UNROLL)
        b, g = group // KVH, group % KVH
        rows = pl.ds(pl.multiple_of(b * BLK, BLK), BLK)
        for h in range(GROUP):
            lanes = pl.ds(pl.multiple_of((g * GROUP + h) * HD, HD), HD)
            dq_s[rows, lanes] = dq_acc[h * BLK : (h + 1) * BLK, :] * SCALE
        return carry

    def back_copy(send, got, index, device):
        return pltpu.make_async_remote_copy(
            src_ref=send.at[pl.ds(CAP * (device[0] * 16 + device[1]), CAP)],
            dst_ref=got.at[pl.ds(CAP * me, CAP)],
            send_sem=send_sem.at[index],
            recv_sem=recv_sem.at[index],
            device_id=device,
            device_id_type=MESH,
        )

    def backward(send, got, index):
        def body(turn, carry):
            devices = peers(turn)
            for a, b in devices:
                for c in range(CAP):
                    send[(a * 16 + b) * CAP + c] = terms[pick_of[c, a * 16 + b]]
            for n, device in enumerate(devices):

                @pl.when(((turn > 0) | (n > 0)) & (device[0] * 16 + device[1] < VALID))
                def _():
                    back_copy(send, got, index, device).start()

            return carry

        lax.fori_loop(0, ROUNDS, body, 0)

        @pl.when(me < VALID)
        def _():
            own = pl.ds(CAP * me, CAP)
            pltpu.make_async_copy(send.at[own], got.at[own], own_sem.at[index - 2]).start()

    def wait_backward(send, got, index):
        @pl.when(me < VALID)
        def _():
            own = pl.ds(CAP * me, CAP)
            pltpu.make_async_copy(send.at[own], got.at[own], own_sem.at[index - 2]).wait()
            wait_bytes(got.at[pl.ds(0, (DEVICES - 1) * CAP)], recv_sem.at[index])
            wait_bytes(send.at[pl.ds(0, SLOTS - CAP)], send_sem.at[index])

        @pl.when(me >= VALID)
        def _():
            wait_bytes(send.at[pl.ds(0, SLOTS)], send_sem.at[index])

    def wait_sent(send, index):
        @pl.when(me < VALID)
        def _():
            wait_bytes(send.at[pl.ds(0, (DEVICES - 1) * CAP)], send_sem.at[index])

    for move in moves:
        move.wait()
    wait_bytes(kl, load_sem.at[0])
    pl.semaphore_wait(barrier, DEVICES - 1)
    forward(kl, sendk, rk, 0)
    wait_bytes(vl, load_sem.at[1])
    forward(vl, sendv, rv, 1)
    load_q.wait()
    load_o.wait()
    wait_forward(rk, 0)
    lax.fori_loop(0, SETS, first_phase, 0)
    wait_sent(sendk, 0)
    backward(sendk, gv_hbm, 2)
    wait_forward(rv, 1)
    lax.fori_loop(0, SETS, second_phase, 0)
    wait_sent(sendv, 1)
    backward(sendv, gk_hbm, 3)
    store_dq = pltpu.make_async_copy(dq_s, dq_hbm, load_sem.at[2])
    store_dq.start()
    wait_backward(sendk, gv_hbm, 2)
    wait_backward(sendv, gk_hbm, 3)
    store_dq.wait()


def exchange(picks, queries, keys, values, d_out):
    anywhere = pl.BlockSpec(memory_space=pl.ANY)
    half, full = jnp.bfloat16, jnp.float32
    table = jax.ShapeDtypeStruct((CAP, DEVICES), jnp.int32)
    back = jax.ShapeDtypeStruct((DEVICES * CAP, BLK, HD), half)
    return pl.pallas_call(
        exchange_kernel,
        out_shape=(jax.ShapeDtypeStruct((QB_DEV * BLK, H * HD), full), back, back, table),
        in_specs=[anywhere] * 5,
        out_specs=[anywhere] * 4,
        scratch_shapes=[
            pltpu.VMEM((DEVICES, PICKS), jnp.int32),
            pltpu.VMEM((CAP, DEVICES), jnp.int32),
            pltpu.VMEM((CAP, DEVICES), jnp.int32),
            pltpu.VMEM((1, PICKS), jnp.int32),
            pltpu.SMEM((CAP, DEVICES), jnp.int32),
            pltpu.SMEM((CAP, DEVICES), jnp.int32),
            pltpu.SMEM((1, PICKS), jnp.int32),
            pltpu.VMEM((TILES, BLK, HD), half),
            pltpu.VMEM((TILES, BLK, HD), half),
            pltpu.VMEM((DEVICES * CAP, BLK, HD), half),
            pltpu.VMEM((DEVICES * CAP, BLK, HD), half),
            pltpu.VMEM((SLOTS, BLK, HD), half),
            pltpu.VMEM((SLOTS, BLK, HD), half),
            pltpu.VMEM((QB_DEV * BLK, H * HD), half),
            pltpu.VMEM((QB_DEV * BLK, H * HD), half),
            pltpu.VMEM((SETS, KEYS, ROWS), full),
            pltpu.VMEM((SETS, 1, ROWS), full),
            pltpu.VMEM((KEYS, ROWS), full),
            pltpu.VMEM((KEYS, HD), half),
            pltpu.VMEM((KEYS, HD), half),
            pltpu.VMEM((ROWS, HD), half),
            pltpu.VMEM((ROWS, HD), half),
            pltpu.VMEM((PICKS, BLK, HD), half),
            pltpu.VMEM((ROWS, HD), full),
            pltpu.VMEM((QB_DEV * BLK, H * HD), full),
            pltpu.SemaphoreType.DMA((8,)),
            pltpu.SemaphoreType.DMA((4,)),
            pltpu.SemaphoreType.DMA((4,)),
            pltpu.SemaphoreType.DMA((2,)),
        ],
        compiler_params=pltpu.CompilerParams(
            collective_id=0, has_side_effects=True, vmem_limit_bytes=62 * MIB
        ),
    )(picks, queries, keys, values, d_out)


FOLD = 32
STEPS = DEVICES * CAP // FOLD


def collect_kernel(
    tile_of, gk_hbm, gv_hbm, dq_hbm, dq_out, dk_out, dv_out,
    gk, gv, dk, dk2, dv, dv2, dq, load_sem, sems,
):
    def load(step):
        part = pl.ds(pl.multiple_of(step * FOLD, FOLD), FOLD)
        return (
            pltpu.make_async_copy(gk_hbm.at[part], gk.at[part], load_sem.at[0, step]),
            pltpu.make_async_copy(gv_hbm.at[part], gv.at[part], load_sem.at[1, step]),
        )

    for step in range(STEPS):
        for copy in load(step):
            copy.start()
    load_dq = pltpu.make_async_copy(dq_hbm, dq, sems.at[2])
    store_dq = pltpu.make_async_copy(dq, dq_out, sems.at[3])
    load_dq.start()
    for part in (dk, dk2, dv, dv2):
        part[...] = jnp.zeros_like(part)

    def fold(step, carry):
        for copy in load(step):
            copy.wait()

        def add(i, carry):
            device = step * (FOLD // CAP) + i
            slot = device * CAP
            tile, tile2 = tile_of[0, device], tile_of[1, device]
            dk[tile] += gk[slot].astype(jnp.float32)
            dk2[tile2] += gk[slot + 1].astype(jnp.float32)
            dv[tile] += gv[slot].astype(jnp.float32)
            dv2[tile2] += gv[slot + 1].astype(jnp.float32)
            return carry

        return lax.fori_loop(0, FOLD // CAP, add, carry, unroll=4)

    lax.fori_loop(0, STEPS, fold, 0)
    load_dq.wait()
    store_dq.start()

    def put(t):
        rows = pl.ds(pl.multiple_of(t // KVH * BLK, BLK), BLK)
        lanes = pl.ds(pl.multiple_of(t % KVH * HD, HD), HD)
        pltpu.make_async_copy(dk.at[t], dk_out.at[rows, lanes], sems.at[0]).start()
        pltpu.make_async_copy(dv.at[t], dv_out.at[rows, lanes], sems.at[1]).start()

    def total(t, carry):
        dk[t] += dk2[t]
        dv[t] += dv2[t]

        @pl.when(t > 0)
        def _():
            put(t - 1)

        return carry

    lax.fori_loop(0, TILES, total, 0)
    put(TILES - 1)
    pltpu.make_async_copy(dk_out, dk_out, sems.at[0]).wait()
    pltpu.make_async_copy(dv_out, dv_out, sems.at[1]).wait()
    store_dq.wait()


def collect(tile_of, gk, gv, d_queries):
    half, full = jnp.bfloat16, jnp.float32
    shape = jax.ShapeDtypeStruct((KB_DEV * BLK, KVH * HD), full)
    anywhere = pl.BlockSpec(memory_space=pl.ANY)
    return pl.pallas_call(
        collect_kernel,
        out_shape=(jax.ShapeDtypeStruct(d_queries.shape, full), shape, shape),
        in_specs=[pl.BlockSpec(memory_space=pltpu.SMEM)] + [anywhere] * 3,
        out_specs=[anywhere] * 3,
        scratch_shapes=[pltpu.VMEM(gk.shape, half)] * 2
        + [pltpu.VMEM((TILES + 1, BLK, HD), full)] * 4
        + [
            pltpu.VMEM(d_queries.shape, full),
            pltpu.SemaphoreType.DMA((2, STEPS)),
            pltpu.SemaphoreType.DMA((4,)),
        ],
        compiler_params=pltpu.CompilerParams(vmem_limit_bytes=62 * MIB),
    )(tile_of, gk, gv, d_queries)


def body(queries, keys, values, d_out, selection):
    picks = selection.reshape(DEVICES, PICKS)
    d_queries, gk, gv, tile_of = exchange(picks, queries, keys, values, d_out)
    return collect(tile_of, gk, gv, d_queries)


def solution(mesh):
    rows = P(("cx", "cy"), None)
    return jax.shard_map(
        body,
        mesh=mesh,
        in_specs=(rows, rows, rows, rows, P()),
        out_specs=(rows, rows, rows),
        check_vma=False,
    )
```

```python
import jax
import jax.numpy as jnp
from jax import lax
from jax.experimental import pallas as pl
from jax.experimental.pallas import tpu as pltpu
from jax.sharding import PartitionSpec as P

H = 32
KVH = 4
HD = 128
BLK = 64
TOPK = 16
QB_DEV = 3
KB_DEV = 16
GROUP = 8
PICKS = 192
CAP = 2
DEVICES = 128
VALID = DEVICES * (KB_DEV - QB_DEV) // KB_DEV
SLOTS = VALID * CAP
TILES = KB_DEV * KVH
SETS = QB_DEV * KVH
KEYS = TOPK * BLK
ROWS = GROUP * BLK
CHUNK = 256
CHUNKS = KEYS // CHUNK
UNROLL = True
SCALE = HD**-0.5
EXP2_SCALE = SCALE * 1.4426950408889634
MESH = pl.DeviceIdType.MESH
MIB = 1024 * 1024


def fill_tables(me, picks, tile_of, pick_of, chosen):
    rows = lax.broadcasted_iota(jnp.int32, (DEVICES, PICKS), 0)
    chosen[...] = jnp.sum(jnp.where(rows == me, picks, 0), axis=0, keepdims=True)
    shape = (PICKS, DEVICES)
    position = lax.broadcasted_iota(jnp.int32, shape, 0)
    device = lax.broadcasted_iota(jnp.int32, shape, 1)
    block = picks.T
    mine = block // KB_DEV == me
    code = position * TILES + block % KB_DEV * KVH + position // TOPK % KVH
    big = PICKS * TILES
    first = jnp.min(jnp.where(mine, code, big), axis=0, keepdims=True)
    last = jnp.max(jnp.where(mine, code, -1), axis=0, keepdims=True)
    tile_of[0:1, :] = jnp.where(first < big, first % TILES, TILES)
    tile_of[1:2, :] = jnp.where(last > first, last % TILES, TILES)
    own = jnp.sum(jnp.where(device == me, block, 0), axis=1, keepdims=True)
    held = own // KB_DEV == device
    pick_of[0:1, :] = jnp.min(jnp.where(held, position, PICKS - 1), axis=0, keepdims=True)
    pick_of[1:2, :] = jnp.max(jnp.where(held, position, 0), axis=0, keepdims=True)


STRIDES = [(0, 0)] + [(a, b) for b in (2, 1, 3, 0) for a in (2, 1, 3, 0)][:-1]
ROUNDS = DEVICES // len(STRIDES)


def exchange_kernel(
    picks_hbm, q_hbm, k_hbm, v_hbm, o_hbm,
    dq_hbm, gk_hbm, gv_hbm, tile_hbm,
    picks, tile_v, pick_v, chosen_v, tile_of, pick_of, chosen,
    kl, vl, sendk, sendv, rk, rv, q_s, o_s, e_s, inv_s, dp_s, kg, vg, qg, og,
    terms, dq_acc, dq_s,
    load_sem, send_sem, recv_sem, own_sem,
):
    cx, cy = lax.axis_index("cx"), lax.axis_index("cy")
    me = cx * 16 + cy
    sign = 1 + 2 * (cx % 2)
    at_x = [(cy + a * sign) % 4 for a in range(4)]
    at_z = [(cy // 4 + b * sign) % 4 * 4 for b in range(4)]

    def peers(turn):
        core = (cx + turn // 4) % 2
        y = [(cx // 2 + (turn % 4 + e) * sign) % 4 * 2 + core for e in range(4)]
        return [(y[(a + b) % 4], at_z[(a + b) % 4] + at_x[a]) for a, b in STRIDES]

    def load_tiles(src, dst, sem):
        def body(t, carry):
            rows = pl.ds(pl.multiple_of(t // KVH * BLK, BLK), BLK)
            lanes = pl.ds(pl.multiple_of(t % KVH * HD, HD), HD)
            pltpu.make_async_copy(src.at[rows, lanes], dst.at[t], sem).start()
            return carry

        lax.fori_loop(0, TILES, body, 0)

    def wait_bytes(ref, sem):
        pltpu.make_async_copy(ref, ref, sem).wait()

    def greet(turn, carry):
        for n, device in enumerate(peers(turn)):

            @pl.when((turn > 0) | (n > 0))
            def _():
                pl.semaphore_signal(barrier, inc=1, device_id=device, device_id_type=MESH)

        return carry

    barrier = pltpu.get_barrier_semaphore()
    load_picks = pltpu.make_async_copy(picks_hbm, picks, load_sem.at[4])
    load_picks.start()
    lax.fori_loop(0, ROUNDS, greet, 0)
    load_tiles(k_hbm, kl, load_sem.at[0])
    load_tiles(v_hbm, vl, load_sem.at[1])
    load_q = pltpu.make_async_copy(q_hbm, q_s, load_sem.at[2])
    load_o = pltpu.make_async_copy(o_hbm, o_s, load_sem.at[3])
    load_q.start()
    load_o.start()
    load_picks.wait()
    fill_tables(me, picks[...], tile_v, pick_v, chosen_v)
    moves = [
        pltpu.make_async_copy(tile_v, tile_of, load_sem.at[4]),
        pltpu.make_async_copy(pick_v, pick_of, load_sem.at[5]),
        pltpu.make_async_copy(chosen_v, chosen, load_sem.at[6]),
        pltpu.make_async_copy(tile_v, tile_hbm, load_sem.at[7]),
    ]
    for move in moves:
        move.start()

    def forward_copy(send, got, index, device):
        return pltpu.make_async_remote_copy(
            src_ref=send.at[pl.ds(CAP * (device[0] * 16 + device[1]), CAP)],
            dst_ref=got.at[pl.ds(CAP * me, CAP)],
            send_sem=send_sem.at[index],
            recv_sem=recv_sem.at[index],
            device_id=device,
            device_id_type=MESH,
        )

    def forward(local, send, got, index):
        @pl.when(me < VALID)
        def _():
            for c in range(CAP):
                tile = jnp.minimum(tile_of[c, me], TILES - 1)
                got[me * CAP + c] = local[tile]

            def body(turn, carry):
                devices = peers(turn)
                for a, b in devices:
                    for c in range(CAP):
                        tile = jnp.minimum(tile_of[c, a * 16 + b], TILES - 1)
                        send[(a * 16 + b) * CAP + c] = local[tile]
                for n, device in enumerate(devices):

                    @pl.when((turn > 0) | (n > 0))
                    def _():
                        forward_copy(send, got, index, device).start()

                return carry

            lax.fori_loop(0, ROUNDS, body, 0)

    def wait_forward(got, index):
        @pl.when(me < VALID)
        def _():
            wait_bytes(got.at[pl.ds(0, SLOTS - CAP)], recv_sem.at[index])

        @pl.when(me >= VALID)
        def _():
            wait_bytes(got, recv_sem.at[index])

    def gather(got, dst, group):
        def body(j, carry):
            rows = pl.ds(pl.multiple_of(j * BLK, BLK), BLK)
            owner = chosen[0, group * TOPK + j] // KB_DEV
            later = (pick_of[0, owner] != group * TOPK + j).astype(jnp.int32)
            dst[rows, :] = got[owner * CAP + later]
            return carry

        lax.fori_loop(0, TOPK, body, 0)

    def rows_of(src, dst, group):
        b, g = group // KVH, group % KVH
        rows = pl.ds(pl.multiple_of(b * BLK, BLK), BLK)
        for h in range(GROUP):
            lanes = pl.ds(pl.multiple_of((g * GROUP + h) * HD, HD), HD)
            dst[h * BLK : (h + 1) * BLK, :] = src[rows, lanes]

    def chunk(c):
        return pl.ds(pl.multiple_of(c * CHUNK, CHUNK), CHUNK)

    def first_phase(group, carry):
        rows_of(q_s, qg, group)
        rows_of(o_s, og, group)
        gather(rk, kg, group)

        def score(c, top):
            s = lax.dot_general(
                kg[chunk(c), :], qg[...], (((1,), (1,)), ((), ())),
                preferred_element_type=jnp.float32,
            )
            e_s[group, chunk(c), :] = s
            return jnp.maximum(top, jnp.max(s, axis=0, keepdims=True))

        top = lax.fori_loop(
            0, CHUNKS, score, jnp.full((1, ROWS), -jnp.inf, jnp.float32), unroll=UNROLL
        )

        def exponent(c, total):
            e = jnp.exp2((e_s[group, chunk(c), :] - top) * EXP2_SCALE)
            e_s[group, chunk(c), :] = e
            return total + jnp.sum(e, axis=0, keepdims=True)

        total = lax.fori_loop(
            0, CHUNKS, exponent, jnp.zeros((1, ROWS), jnp.float32), unroll=UNROLL
        )
        inverse = 1.0 / total
        inv_s[group] = inverse

        def value_terms(c, carry):
            p = (e_s[group, chunk(c), :] * inverse).astype(jnp.bfloat16)
            dv = jnp.dot(p, og[...], preferred_element_type=jnp.float32)
            n = CHUNK // BLK
            terms[pl.ds(group * TOPK + c * n, n)] = dv.astype(jnp.bfloat16).reshape(n, BLK, HD)
            return carry

        return lax.fori_loop(0, CHUNKS, value_terms, carry, unroll=UNROLL)

    def second_phase(group, carry):
        rows_of(q_s, qg, group)
        rows_of(o_s, og, group)
        gather(rk, kg, group)
        gather(rv, vg, group)

        def d_prob(c, delta):
            dp = lax.dot_general(
                vg[chunk(c), :], og[...], (((1,), (1,)), ((), ())),
                preferred_element_type=jnp.float32,
            )
            dp_s[chunk(c), :] = dp
            return delta + jnp.sum(e_s[group, chunk(c), :] * dp, axis=0, keepdims=True)

        delta = lax.fori_loop(
            0, CHUNKS, d_prob, jnp.zeros((1, ROWS), jnp.float32), unroll=UNROLL
        )
        inverse = inv_s[group]
        delta = delta * inverse
        dq_acc[...] = jnp.zeros_like(dq_acc)

        def key_terms(c, carry):
            p = e_s[group, chunk(c), :] * inverse
            ds = (p * (dp_s[chunk(c), :] - delta)).astype(jnp.bfloat16)
            dk = jnp.dot(ds, qg[...], preferred_element_type=jnp.float32) * SCALE
            n = CHUNK // BLK
            terms[pl.ds(group * TOPK + c * n, n)] = dk.astype(jnp.bfloat16).reshape(n, BLK, HD)
            dq_acc[...] += lax.dot_general(
                ds, kg[chunk(c), :], (((0,), (0,)), ((), ())),
                preferred_element_type=jnp.float32,
            )
            return carry

        lax.fori_loop(0, CHUNKS, key_terms, 0, unroll=UNROLL)
        b, g = group // KVH, group % KVH
        rows = pl.ds(pl.multiple_of(b * BLK, BLK), BLK)
        for h in range(GROUP):
            lanes = pl.ds(pl.multiple_of((g * GROUP + h) * HD, HD), HD)
            dq_s[rows, lanes] = dq_acc[h * BLK : (h + 1) * BLK, :] * SCALE
        return carry

    def back_copy(send, got, index, device):
        return pltpu.make_async_remote_copy(
            src_ref=send.at[pl.ds(CAP * (device[0] * 16 + device[1]), CAP)],
            dst_ref=got.at[pl.ds(CAP * me, CAP)],
            send_sem=send_sem.at[index],
            recv_sem=recv_sem.at[index],
            device_id=device,
            device_id_type=MESH,
        )

    def backward(send, got, index):
        def body(turn, carry):
            devices = peers(turn)
            for a, b in devices:
                for c in range(CAP):
                    send[(a * 16 + b) * CAP + c] = terms[pick_of[c, a * 16 + b]]
            for n, device in enumerate(devices):

                @pl.when(((turn > 0) | (n > 0)) & (device[0] * 16 + device[1] < VALID))
                def _():
                    back_copy(send, got, index, device).start()

            return carry

        lax.fori_loop(0, ROUNDS, body, 0)

        @pl.when(me < VALID)
        def _():
            own = pl.ds(CAP * me, CAP)
            pltpu.make_async_copy(send.at[own], got.at[own], own_sem.at[index - 2]).start()

    def wait_backward(send, got, index):
        @pl.when(me < VALID)
        def _():
            own = pl.ds(CAP * me, CAP)
            pltpu.make_async_copy(send.at[own], got.at[own], own_sem.at[index - 2]).wait()
            wait_bytes(got.at[pl.ds(0, (DEVICES - 1) * CAP)], recv_sem.at[index])
            wait_bytes(send.at[pl.ds(0, SLOTS - CAP)], send_sem.at[index])

        @pl.when(me >= VALID)
        def _():
            wait_bytes(send.at[pl.ds(0, SLOTS)], send_sem.at[index])

    def wait_sent(send, index):
        @pl.when(me < VALID)
        def _():
            wait_bytes(send.at[pl.ds(0, (DEVICES - 1) * CAP)], send_sem.at[index])

    for move in moves:
        move.wait()
    wait_bytes(kl, load_sem.at[0])
    pl.semaphore_wait(barrier, DEVICES - 1)
    forward(kl, sendk, rk, 0)
    wait_bytes(vl, load_sem.at[1])
    forward(vl, sendv, rv, 1)
    load_q.wait()
    load_o.wait()
    wait_forward(rk, 0)
    lax.fori_loop(0, SETS, first_phase, 0)
    wait_sent(sendk, 0)
    backward(sendk, gv_hbm, 2)
    wait_forward(rv, 1)
    lax.fori_loop(0, SETS, second_phase, 0)
    wait_sent(sendv, 1)
    backward(sendv, gk_hbm, 3)
    store_dq = pltpu.make_async_copy(dq_s, dq_hbm, load_sem.at[2])
    store_dq.start()
    wait_backward(sendk, gv_hbm, 2)
    wait_backward(sendv, gk_hbm, 3)
    store_dq.wait()


def exchange(picks, queries, keys, values, d_out):
    anywhere = pl.BlockSpec(memory_space=pl.ANY)
    half, full = jnp.bfloat16, jnp.float32
    table = jax.ShapeDtypeStruct((CAP, DEVICES), jnp.int32)
    back = jax.ShapeDtypeStruct((DEVICES * CAP, BLK, HD), half)
    return pl.pallas_call(
        exchange_kernel,
        out_shape=(jax.ShapeDtypeStruct((QB_DEV * BLK, H * HD), full), back, back, table),
        in_specs=[anywhere] * 5,
        out_specs=[anywhere] * 4,
        scratch_shapes=[
            pltpu.VMEM((DEVICES, PICKS), jnp.int32),
            pltpu.VMEM((CAP, DEVICES), jnp.int32),
            pltpu.VMEM((CAP, DEVICES), jnp.int32),
            pltpu.VMEM((1, PICKS), jnp.int32),
            pltpu.SMEM((CAP, DEVICES), jnp.int32),
            pltpu.SMEM((CAP, DEVICES), jnp.int32),
            pltpu.SMEM((1, PICKS), jnp.int32),
            pltpu.VMEM((TILES, BLK, HD), half),
            pltpu.VMEM((TILES, BLK, HD), half),
            pltpu.VMEM((DEVICES * CAP, BLK, HD), half),
            pltpu.VMEM((DEVICES * CAP, BLK, HD), half),
            pltpu.VMEM((SLOTS, BLK, HD), half),
            pltpu.VMEM((SLOTS, BLK, HD), half),
            pltpu.VMEM((QB_DEV * BLK, H * HD), half),
            pltpu.VMEM((QB_DEV * BLK, H * HD), half),
            pltpu.VMEM((SETS, KEYS, ROWS), full),
            pltpu.VMEM((SETS, 1, ROWS), full),
            pltpu.VMEM((KEYS, ROWS), full),
            pltpu.VMEM((KEYS, HD), half),
            pltpu.VMEM((KEYS, HD), half),
            pltpu.VMEM((ROWS, HD), half),
            pltpu.VMEM((ROWS, HD), half),
            pltpu.VMEM((PICKS, BLK, HD), half),
            pltpu.VMEM((ROWS, HD), full),
            pltpu.VMEM((QB_DEV * BLK, H * HD), full),
            pltpu.SemaphoreType.DMA((8,)),
            pltpu.SemaphoreType.DMA((4,)),
            pltpu.SemaphoreType.DMA((4,)),
            pltpu.SemaphoreType.DMA((2,)),
        ],
        compiler_params=pltpu.CompilerParams(
            collective_id=0, has_side_effects=True, vmem_limit_bytes=62 * MIB
        ),
    )(picks, queries, keys, values, d_out)


FOLD = 32
STEPS = DEVICES * CAP // FOLD


def collect_kernel(
    tile_of, gk_hbm, gv_hbm, dq_hbm, dq_out, dk_out, dv_out,
    gk, gv, dk, dk2, dv, dv2, dq, load_sem, sems,
):
    def load(step):
        part = pl.ds(pl.multiple_of(step * FOLD, FOLD), FOLD)
        return (
            pltpu.make_async_copy(gk_hbm.at[part], gk.at[part], load_sem.at[0, step]),
            pltpu.make_async_copy(gv_hbm.at[part], gv.at[part], load_sem.at[1, step]),
        )

    for step in range(STEPS):
        for copy in load(step):
            copy.start()
    load_dq = pltpu.make_async_copy(dq_hbm, dq, sems.at[2])
    store_dq = pltpu.make_async_copy(dq, dq_out, sems.at[3])
    load_dq.start()
    for part in (dk, dk2, dv, dv2):
        part[...] = jnp.zeros_like(part)

    def fold(step, carry):
        for copy in load(step):
            copy.wait()

        def add(i, carry):
            device = step * (FOLD // CAP) + i
            slot = device * CAP
            tile, tile2 = tile_of[0, device], tile_of[1, device]
            dk[tile] += gk[slot].astype(jnp.float32)
            dk2[tile2] += gk[slot + 1].astype(jnp.float32)
            dv[tile] += gv[slot].astype(jnp.float32)
            dv2[tile2] += gv[slot + 1].astype(jnp.float32)
            return carry

        return lax.fori_loop(0, FOLD // CAP, add, carry, unroll=4)

    lax.fori_loop(0, STEPS, fold, 0)
    load_dq.wait()
    store_dq.start()

    def put(t):
        rows = pl.ds(pl.multiple_of(t // KVH * BLK, BLK), BLK)
        lanes = pl.ds(pl.multiple_of(t % KVH * HD, HD), HD)
        pltpu.make_async_copy(dk.at[t], dk_out.at[rows, lanes], sems.at[0]).start()
        pltpu.make_async_copy(dv.at[t], dv_out.at[rows, lanes], sems.at[1]).start()

    def total(t, carry):
        dk[t] += dk2[t]
        dv[t] += dv2[t]

        @pl.when(t > 0)
        def _():
            put(t - 1)

        return carry

    lax.fori_loop(0, TILES, total, 0)
    put(TILES - 1)
    pltpu.make_async_copy(dk_out, dk_out, sems.at[0]).wait()
    pltpu.make_async_copy(dv_out, dv_out, sems.at[1]).wait()
    store_dq.wait()


def collect(tile_of, gk, gv, d_queries):
    half, full = jnp.bfloat16, jnp.float32
    shape = jax.ShapeDtypeStruct((KB_DEV * BLK, KVH * HD), full)
    anywhere = pl.BlockSpec(memory_space=pl.ANY)
    return pl.pallas_call(
        collect_kernel,
        out_shape=(jax.ShapeDtypeStruct(d_queries.shape, full), shape, shape),
        in_specs=[pl.BlockSpec(memory_space=pltpu.SMEM)] + [anywhere] * 3,
        out_specs=[anywhere] * 3,
        scratch_shapes=[pltpu.VMEM(gk.shape, half)] * 2
        + [pltpu.VMEM((TILES + 1, BLK, HD), full)] * 4
        + [
            pltpu.VMEM(d_queries.shape, full),
            pltpu.SemaphoreType.DMA((2, STEPS)),
            pltpu.SemaphoreType.DMA((4,)),
        ],
        compiler_params=pltpu.CompilerParams(vmem_limit_bytes=62 * MIB),
    )(tile_of, gk, gv, d_queries)


def body(queries, keys, values, d_out, selection):
    picks = selection.reshape(DEVICES, PICKS)
    d_queries, gk, gv, tile_of = exchange(picks, queries, keys, values, d_out)
    return collect(tile_of, gk, gv, d_queries)


def solution(mesh):
    rows = P(("cx", "cy"), None)
    return jax.shard_map(
        body,
        mesh=mesh,
        in_specs=(rows, rows, rows, rows, P()),
        out_specs=(rows, rows, rows),
        check_vma=False,
    )
```
